256 devices in a mesh: cells: 32 (over y, z), bins: 8 (over x, core).
Axes of the slice: x: 4, y: 4, z: 8, core: 2. Of those that a mesh axis runs over, the one named last changes fastest.
Arguments:
- snapshots: bfloat16 [8, 262144, 512], P('bins', 'cells'), may hold values from -150 to 150
- training: int32 [262144], P('cells'), may hold values 0 or 1
- doppler: int32 [8, 128], P('bins'), may hold values from 0 to 1023
Outputs:
- filtered: bfloat16 [8, 256, 262144], P('bins', None, 'cells')
The draws below stay inside these ranges and needn't reach their ends.
All inputs are finite; a program needn't handle non-finite values. No bound on the sum of `training` on one device may be relied on, other than what follows from the above.
Results may differ from the reference program's by a relative error of at most 0.003.
The reference program's roundings to bfloat16 on the way (of `taps`) count: a program that leaves them out, or rounds other values in their place, can miss the bound.
Values sent between devices are 32-bit elements; how exact they have to be, the bound alone decides.
No kernel may reach another device: no remote copies, remote signals or barrier semaphores. Data moves between devices by JAX's collectives and lax.ppermute only.
A program may use at most 64 MiB of HBM per device.

```python
import jax
import jax.numpy as jnp
from jax import lax

CHANNELS = 16
PULSES = 16
DIM = 256
BINS_G = 128
NDOPP = 1024
CELLS = 262144
GROUPS = 8


def draw_snapshots(key, part):
    keys = jax.random.split(jax.random.fold_in(key, 7101), 13)
    patches = CHANNELS + PULSES
    jammers = 2
    width = 2 * DIM
    noise_part = jnp.clip(jax.random.normal(keys[0], (GROUPS, CELLS, width), jnp.float32), -4.0, 4.0)
    clutter_re = jnp.clip(jax.random.normal(keys[1], (GROUPS, CELLS, patches), jnp.float32), -4.0, 4.0) * 0.7071
    clutter_im = jnp.clip(jax.random.normal(keys[2], (GROUPS, CELLS, patches), jnp.float32), -4.0, 4.0) * 0.7071
    jam_re = jnp.clip(jax.random.normal(keys[3], (GROUPS, CELLS, jammers, PULSES), jnp.float32), -4.0, 4.0) * 0.7071
    jam_im = jnp.clip(jax.random.normal(keys[4], (GROUPS, CELLS, jammers, PULSES), jnp.float32), -4.0, 4.0) * 0.7071
    gains = jnp.exp(jax.random.uniform(keys[5], (GROUPS, 1, DIM), jnp.float32, jnp.log(0.5), jnp.log(2.0)))
    index = jnp.arange(DIM)
    chan = (index // PULSES).astype(jnp.float32)
    pulse = (index % PULSES).astype(jnp.float32)
    offset = jax.random.uniform(keys[6], (GROUPS, 1), jnp.float32, 0.0, 1.0)
    spatial = (jnp.arange(patches).astype(jnp.float32)[None, :] + offset) / patches - 0.5
    slope = jax.random.uniform(keys[7], (GROUPS, 1), jnp.float32, 0.8, 1.2)
    temporal = slope * spatial
    phase = 2.0 * jnp.pi * (spatial[:, :, None] * chan[None, None, :] + temporal[:, :, None] * pulse[None, None, :])
    patch_power = jnp.exp(jax.random.uniform(keys[8], (GROUPS, 1, patches), jnp.float32, jnp.log(0.5), jnp.log(8.0)))
    amp_re = clutter_re * jnp.sqrt(patch_power)
    amp_im = clutter_im * jnp.sqrt(patch_power)
    cosines = jnp.cos(phase)
    sines = jnp.sin(phase)
    real_sum = jnp.einsum('gnk,gkd->gnd', amp_re, cosines) - jnp.einsum('gnk,gkd->gnd', amp_im, sines)
    imag_sum = jnp.einsum('gnk,gkd->gnd', amp_re, sines) + jnp.einsum('gnk,gkd->gnd', amp_im, cosines)
    jam_angle = jax.random.uniform(keys[9], (GROUPS, jammers), jnp.float32, -0.5, 0.5)
    jam_power = jnp.exp(jax.random.uniform(keys[10], (GROUPS, 1, jammers, 1), jnp.float32, jnp.log(10.0), jnp.log(60.0)))
    chans = jnp.arange(CHANNELS).astype(jnp.float32)
    jam_phase = 2.0 * jnp.pi * jam_angle[:, :, None] * chans[None, None, :]
    jam_cos = jnp.cos(jam_phase)
    jam_sin = jnp.sin(jam_phase)
    jr = jam_re * jnp.sqrt(jam_power)
    ji = jam_im * jnp.sqrt(jam_power)
    jam_real = jnp.einsum('gnjp,gjc->gncp', jr, jam_cos) - jnp.einsum('gnjp,gjc->gncp', ji, jam_sin)
    jam_imag = jnp.einsum('gnjp,gjc->gncp', jr, jam_sin) + jnp.einsum('gnjp,gjc->gncp', ji, jam_cos)
    real_sum = real_sum + jam_real.reshape(GROUPS, CELLS, DIM)
    imag_sum = imag_sum + jam_imag.reshape(GROUPS, CELLS, DIM)
    signal = jnp.concatenate([real_sum, imag_sum], -1) + noise_part
    both_gains = jnp.concatenate([gains, gains], -1)
    rough = jnp.exp(jax.random.uniform(keys[11], (GROUPS, CELLS, 1), jnp.float32, 0.0, jnp.log(3.0)))
    place = jnp.arange(CELLS).astype(jnp.float32) / CELLS
    ranged = (0.6 + 1.4 * place)[None, :, None]
    order = jax.random.permutation(keys[12], GROUPS).astype(jnp.float32)
    level = (1.0 + 2.0 * order / max(GROUPS - 1, 1))[:, None, None]
    return jnp.clip(0.15 * signal * both_gains * rough * ranged * level, -150.0, 150.0).astype(jnp.bfloat16)


def plant(array, key, low, top_value):
    longest = array.shape.index(max(array.shape))
    spots = []
    for shift in (0, 1):
        where = [jax.random.randint(jax.random.fold_in(key, axis), (), 0, length) for axis, length in enumerate(array.shape)]
        where[longest] = (where[longest] + shift) % array.shape[longest]
        spots.append(tuple(where))
    return array.at[spots[0]].set(low).at[spots[1]].set(top_value)


def setup_inputs(seed: int = 0) -> dict:
    seeds = jax.random.split(jax.random.key(seed), 4)
    snapshots = draw_snapshots(jax.random.fold_in(seeds[3], 71), 0)
    training = plant((jax.random.randint(seeds[1], (CELLS,), 0, 4) < 3).astype(jnp.int32), jax.random.fold_in(seeds[1], 1), 0, 1)
    doppler = plant(jax.random.randint(seeds[2], (GROUPS, BINS_G), 0, NDOPP), jax.random.fold_in(seeds[2], 1), 0, NDOPP - 1).astype(jnp.int32)
    return {"snapshots": snapshots, "training": training, "doppler": doppler}


load_ratio = 0.5
look_freq = 0.125

def steering(doppler):
    index = jnp.arange(CHANNELS * PULSES)
    chan = (index // PULSES).astype(jnp.float32)
    pulse = (index % PULSES).astype(jnp.float32)
    freq = doppler.astype(jnp.float32) / NDOPP - 0.5
    phase = 2.0 * jnp.pi * (look_freq * chan[:, None] + pulse[:, None] * freq[None, :])
    return jnp.concatenate([jnp.cos(phase), jnp.sin(phase)], 0) / jnp.sqrt(jnp.float32(DIM))

def complex_parts(gram):
    half = gram.shape[0] // 2
    upper = gram[:half, :half]
    cross = gram[:half, half:]
    lower = gram[half:, half:]
    return (upper + lower, cross.T - cross)

def filter_group(real_part, imag_part, noise, doppler, snaps):
    half = real_part.shape[0]
    loaded = real_part + load_ratio * noise * jnp.eye(half, dtype=jnp.float32)
    embed = jnp.concatenate([jnp.concatenate([loaded, -imag_part], 1), jnp.concatenate([imag_part, loaded], 1)], 0)
    factor = jnp.linalg.cholesky(embed)
    steer = steering(doppler)
    weights = jax.scipy.linalg.cho_solve((factor, True), steer)
    gain = lax.optimization_barrier(jnp.sum(steer * weights, axis=0))
    w_real = weights[:half] / gain[None, :]
    w_imag = weights[half:] / gain[None, :]
    taps = jnp.concatenate([jnp.concatenate([w_real, w_imag], 0), jnp.concatenate([-w_imag, w_real], 0)], 1).astype(jnp.bfloat16)
    result = lax.dot_general(taps.astype(jnp.float32), snaps.astype(jnp.float32), (((0,), (1,)), ((), ())), preferred_element_type=jnp.float32)
    return result.astype(jnp.bfloat16)

def reference(snapshots, training, doppler):
    keep = training.astype(jnp.bfloat16)[:, None]
    parts = []
    power = jnp.float32(0.0)
    for group in range(GROUPS):
        snaps = snapshots[group]
        gram = lax.dot_general((snaps * keep).astype(jnp.float32), snaps.astype(jnp.float32), (((0,), (0,)), ((), ())), preferred_element_type=jnp.float32)
        real_part, imag_part = complex_parts(gram)
        parts.append((real_part, imag_part))
        power = power + jnp.trace(real_part)
    noise = power / (GROUPS * DIM)
    outputs = []
    for group in range(GROUPS):
        outputs.append(filter_group(parts[group][0], parts[group][1], noise, doppler[group], snapshots[group]))
    return jnp.stack(outputs)
```

```python
import functools

import jax
import jax.numpy as jnp
from jax import lax
from jax.experimental import pallas as pl
from jax.experimental.pallas import tpu as pltpu
from jax.sharding import PartitionSpec as P

CHANNELS = 16
PULSES = 16
NDOPP = 1024
LANES = 128
GRAM_CELLS = 1024
FILTER_CELLS = 1024

load_ratio = 0.5
look_freq = 0.125

bf16 = jnp.bfloat16
f32 = jnp.float32


def dot(a, b):
    return jnp.dot(a, b, preferred_element_type=f32)


def gram_body(x_ref, keep_ref, out_ref, acc_ref):
    step = pl.program_id(0)
    half = x_ref.shape[1] // 2

    @pl.when(step == 0)
    def _():
        acc_ref[...] = jnp.zeros_like(acc_ref)

    x = x_ref[...]
    kept = x.T * keep_ref[...].astype(f32).astype(bf16)
    by_real = dot(kept, x[:, :half])
    by_imag = dot(kept[half:], x[:, half:])
    acc_ref[:half] += by_real[:half] + by_imag
    acc_ref[half:] += by_real[half:]

    @pl.when(step == pl.num_programs(0) - 1)
    def _():
        real = acc_ref[:half]
        cross = acc_ref[half:]
        imag = cross - cross.T
        rows = lax.broadcasted_iota(jnp.int32, (half, half), 0)
        cols = lax.broadcasted_iota(jnp.int32, (half, half), 1)
        packed = jnp.where(rows <= cols, real, imag)
        trace = jnp.sum(jnp.where(rows == cols, real, 0.0), keepdims=True)
        parts = half // 8
        span = out_ref.shape[0] // parts
        for part in range(parts):
            lines = packed[8 * part : 8 * part + 8]
            for block in range(half // LANES):
                out_ref[span * part + 8 * block : span * part + 8 * block + 8] = lines[
                    :, LANES * block : LANES * block + LANES
                ]
            out_ref[span * part + span - 1 : span * part + span] = jnp.broadcast_to(trace, (1, LANES))


def local_gram(snaps, keep):
    cells, width = snaps.shape
    half = width // 2
    span = 8 * half // LANES + 1
    return pl.pallas_call(
        gram_body,
        grid=(cells // GRAM_CELLS,),
        in_specs=[
            pl.BlockSpec((GRAM_CELLS, width), lambda i: (i, 0)),
            pl.BlockSpec((1, GRAM_CELLS), lambda i: (0, i)),
        ],
        out_specs=pl.BlockSpec((half // 8 * span, LANES), lambda i: (0, 0)),
        out_shape=jax.ShapeDtypeStruct((half // 8 * span, LANES), f32),
        scratch_shapes=[pltpu.VMEM((width, half), f32)],
        name="gram",
    )(snaps, keep)


def halves(x):
    top = x.astype(bf16)
    return top, (x - top.astype(f32)).astype(bf16)


def three(ah, al, bh, bl):
    return dot(jnp.concatenate([ah, ah, al], 1), jnp.concatenate([bh, bl, bh], 0))


def solve_body(gathered_ref, power_ref, sr_ref, si_ref, out_ref, ar, ai, er, ei, xr, xi):
    n = ar.shape[0]
    lines = gathered_ref[...].reshape(n // 8, n // LANES, 8, LANES)
    p = jnp.concatenate([lines[:, b].reshape(n, LANES) for b in range(n // LANES)], 1)
    rows = lax.broadcasted_iota(jnp.int32, (n, n), 0)
    cols = lax.broadcasted_iota(jnp.int32, (n, n), 1)
    eye = rows == cols
    pt = p.T
    re = jnp.where(rows <= cols, p, pt)
    im = jnp.where(rows > cols, p, jnp.where(rows < cols, -pt, 0.0))
    squares = 2.0 * p * p - jnp.where(eye, p * p, 0.0)
    low = load_ratio * power_ref[0:1, 0:1]
    high = jnp.sqrt(jnp.sum(squares, keepdims=True)) + low
    alpha = 2.0 / (low + high)
    rho = ((high - low) / (high + low))[0, 0]
    full = jnp.where(eye, re + low, re)
    ar[...] = full
    ai[...] = im
    er[...] = jnp.where(eye, 1.0, 0.0) - alpha * full
    ei[...] = -alpha * im
    xr[...] = alpha * jnp.where(eye, 1.0, 0.0)
    xi[...] = jnp.zeros_like(im)

    def step(exact, rho):
        e_r, e_i, x_r, x_i = er[...], ei[...], xr[...], xi[...]
        if exact:
            (rh, rl), (ih, il) = halves(e_r), halves(e_i)
            (xh, xl), (yh, yl) = halves(x_r), halves(x_i)
            top = jnp.concatenate([rh, ih, xh, yh], 1)
            rest = jnp.concatenate([rl, il, xl, yl], 1)
            by_real = three(rh, rl, top, rest)
            by_imag = three(ih, il, top, rest)
        else:
            both = jnp.concatenate([v.astype(bf16) for v in (e_r, e_i, x_r, x_i)], 1)
            by_real = dot(both[:, :n], both)
            by_imag = dot(both[:, n : 2 * n], both)
        mu = 2.0 / (2.0 - rho * rho)
        er[...] = mu * (by_real[:, :n] - by_imag[:, n : 2 * n]) + jnp.where(eye, 1.0 - mu, 0.0)
        ei[...] = mu * (by_real[:, n : 2 * n] + by_imag[:, :n])
        xr[...] = mu * (x_r + by_real[:, 2 * n : 3 * n] - by_imag[:, 3 * n :])
        xi[...] = mu * (x_i + by_real[:, 3 * n :] + by_imag[:, 2 * n : 3 * n])
        return rho * rho * mu * 0.5

    rho = lax.while_loop(lambda r: r > 0.5, functools.partial(step, True), rho)
    lax.while_loop(lambda r: r > 1e-3, functools.partial(step, False), rho)
    s_r, s_i = sr_ref[...], si_ref[...]
    (xh, xl), (yh, yl) = halves(xr[...]), halves(xi[...])
    top = jnp.concatenate([jnp.concatenate([xh, -yh], 1), jnp.concatenate([yh, xh], 1)], 0)
    rest = jnp.concatenate([jnp.concatenate([xl, -yl], 1), jnp.concatenate([yl, xl], 1)], 0)

    def applied(v_r, v_i):
        (rh, rl), (ih, il) = halves(v_r), halves(v_i)
        return three(jnp.concatenate([rh, ih], 1), jnp.concatenate([rl, il], 1), top, rest)

    w = applied(s_r, s_i)
    a = jnp.concatenate(
        [jnp.concatenate([ar[...], -ai[...]], 1), jnp.concatenate([ai[...], ar[...]], 1)], 0
    )
    back = jnp.dot(w, a, precision=lax.Precision.HIGHEST, preferred_element_type=f32)
    w = w + applied(s_r - back[:, :n], s_i - back[:, n:])
    w_r, w_i = w[:, :n], w[:, n:]
    gain = jnp.sum(s_r * w_r + s_i * w_i, axis=1, keepdims=True)
    t_r = (w_r / gain).astype(bf16)
    t_i = (w_i / gain).astype(bf16)
    m = s_r.shape[0]
    out_ref[:m, :n] = t_r
    out_ref[:m, n:] = t_i
    out_ref[m:, :n] = -t_i
    out_ref[m:, n:] = t_r


def solve(gathered, noise, steer_real, steer_imag):
    m, n = steer_real.shape
    return pl.pallas_call(
        solve_body,
        out_shape=jax.ShapeDtypeStruct((2 * m, 2 * n), bf16),
        scratch_shapes=[pltpu.VMEM((n, n), f32)] * 6,
        name="solve",
    )(gathered, noise, steer_real, steer_imag)


def filter_body(taps_ref, x_ref, out_ref):
    out_ref[...] = lax.dot_general(
        taps_ref[...], x_ref[...], (((1,), (1,)), ((), ())), preferred_element_type=f32
    ).astype(bf16)


def filtered(taps, snaps):
    cells, width = snaps.shape
    return pl.pallas_call(
        filter_body,
        grid=(cells // FILTER_CELLS,),
        in_specs=[
            pl.BlockSpec(taps.shape, lambda i: (0, 0)),
            pl.BlockSpec((FILTER_CELLS, width), lambda i: (i, 0)),
        ],
        out_specs=pl.BlockSpec((taps.shape[0], FILTER_CELLS), lambda i: (0, i)),
        out_shape=jax.ShapeDtypeStruct((taps.shape[0], cells), bf16),
        name="filter",
    )(taps, snaps)


def steering(doppler, chans, pulses):
    index = jnp.arange(chans * pulses)
    chan = (index // pulses).astype(f32)
    pulse = (index % pulses).astype(f32)
    freq = doppler.astype(f32) / NDOPP - 0.5
    phase = 2.0 * jnp.pi * (look_freq * chan[None, :] + pulse[None, :] * freq[:, None])
    scale = jnp.sqrt(f32(chans * pulses))
    return jnp.cos(phase) / scale, jnp.sin(phase) / scale


def exchange(x, axis):
    return lax.all_to_all(x, axis, split_axis=0, concat_axis=0, tiled=True)


def sum_of_few(x, axis):
    size = lax.axis_size(axis)
    stride = 1
    while stride < size:
        x = x + lax.ppermute(x, axis, [(i, i ^ stride) for i in range(size)])
        stride *= 2
    return x


def per_device(snapshots, training, doppler):
    snaps = snapshots[0]
    cells, width = snaps.shape
    half = width // 2
    parts = lax.axis_size("cells")
    sums = local_gram(snaps, training.reshape(1, cells))
    own = exchange(sums.reshape(parts, 1, -1), "cells").sum(axis=0)
    count = 8 * half
    lines = own[0, :count].reshape(-1, LANES)
    trace = own[:, count:]
    gathered = exchange(jnp.broadcast_to(lines, (parts, *lines.shape)), "cells")
    power = sum_of_few(trace, "bins")
    noise = power / (lax.axis_size("bins") * half)
    steer_real, steer_imag = steering(doppler[0], CHANNELS, PULSES)
    taps = solve(gathered.reshape(-1, LANES), noise, steer_real, steer_imag)
    return filtered(taps, snaps)[None]


def solution(mesh):
    in_specs = (P("bins", "cells", None), P("cells"), P("bins", None))
    out_specs = P("bins", None, "cells")
    return jax.shard_map(
        per_device, mesh=mesh, in_specs=in_specs, out_specs=out_specs, check_vma=False
    )
```

```python
import functools

import jax
import jax.numpy as jnp
from jax import lax
from jax.experimental import pallas as pl
from jax.experimental.pallas import tpu as pltpu
from jax.sharding import PartitionSpec as P

CHANNELS = 16
PULSES = 16
NDOPP = 1024
LANES = 128
GRAM_CELLS = 2048
GRAM_AHEAD = 4
FILTER_CELLS = 2048

load_ratio = 0.5
look_freq = 0.125

bf16 = jnp.bfloat16
f32 = jnp.float32


def dot(a, b):
    return jnp.dot(a, b, preferred_element_type=f32)


def gram_body(x_hbm, keep_hbm, out_ref, x_ref, keep_ref, acc_ref, sems):
    cells, width = x_ref.shape
    half = width // 2
    steps = cells // GRAM_CELLS

    def copy(step):
        rows = pl.ds(pl.multiple_of(step * GRAM_CELLS, GRAM_CELLS), GRAM_CELLS)
        return pltpu.make_async_copy(x_hbm.at[rows], x_ref.at[rows], sems.at[step])

    copy(0).start()
    keeps = pltpu.make_async_copy(keep_hbm, keep_ref, sems.at[steps])
    keeps.start()
    for step in range(1, GRAM_AHEAD):
        copy(step).start()
    acc_ref[...] = jnp.zeros_like(acc_ref)

    def add(step, _):
        @pl.when(step + GRAM_AHEAD < steps)
        def _():
            copy(step + GRAM_AHEAD).start()

        copy(step).wait()
        start = pl.multiple_of(step * GRAM_CELLS, GRAM_CELLS)
        x = x_ref[pl.ds(start, GRAM_CELLS)]
        keep = keep_ref[:, pl.ds(start, GRAM_CELLS)]
        kept = x.T * keep.astype(f32).astype(bf16)
        by_real = dot(kept, x[:, :half])
        by_imag = dot(kept[half:], x[:, half:])
        acc_ref[:half] += by_real[:half] + by_imag
        acc_ref[half:] += by_real[half:]
        return 0

    keeps.wait()
    lax.fori_loop(0, steps, add, 0)
    real = acc_ref[:half]
    cross = acc_ref[half:]
    imag = cross - cross.T
    rows = lax.broadcasted_iota(jnp.int32, (half, half), 0)
    cols = lax.broadcasted_iota(jnp.int32, (half, half), 1)
    packed = jnp.where(rows <= cols, real, imag)
    trace = jnp.sum(jnp.where(rows == cols, real, 0.0), keepdims=True)
    parts = half // 8
    span = out_ref.shape[0] // parts
    for part in range(parts):
        lines = packed[8 * part : 8 * part + 8]
        for block in range(half // LANES):
            out_ref[span * part + 8 * block : span * part + 8 * block + 8] = lines[
                :, LANES * block : LANES * block + LANES
            ]
        out_ref[span * part + span - 1 : span * part + span] = jnp.broadcast_to(trace, (1, LANES))


def local_gram(snaps, keep):
    cells, width = snaps.shape
    half = width // 2
    span = 8 * half // LANES + 1
    return pl.pallas_call(
        gram_body,
        in_specs=[pl.BlockSpec(memory_space=pl.ANY)] * 2,
        out_specs=pl.BlockSpec(memory_space=pltpu.VMEM),
        out_shape=jax.ShapeDtypeStruct((half // 8 * span, LANES), f32),
        scratch_shapes=[
            pltpu.VMEM((cells, width), bf16),
            pltpu.VMEM((1, cells), jnp.int32),
            pltpu.VMEM((width, half), f32),
            pltpu.SemaphoreType.DMA((cells // GRAM_CELLS + 1,)),
        ],
        name="gram",
    )(snaps, keep)


def halves(x):
    top = x.astype(bf16)
    return top, (x - top.astype(f32)).astype(bf16)


def three(ah, al, bh, bl):
    return dot(jnp.concatenate([ah, ah, al], 1), jnp.concatenate([bh, bl, bh], 0))


def solve_body(
    gathered_ref, power_ref, sr_ref, si_ref, x_hbm, out_hbm, x_ref, out_ref, ar, ai, er, ei, xr, xi, sems
):
    n = ar.shape[0]
    cells = x_ref.shape[0]
    chunks = cells // FILTER_CELLS
    spans = [pl.ds(FILTER_CELLS * i, FILTER_CELLS) for i in range(chunks)]
    arrivals = [
        pltpu.make_async_copy(x_hbm.at[span], x_ref.at[span], sems.at[0, i])
        for i, span in enumerate(spans)
    ]
    lines = gathered_ref[...].reshape(n // 8, n // LANES, 8, LANES)
    p = jnp.concatenate([lines[:, b].reshape(n, LANES) for b in range(n // LANES)], 1)
    rows = lax.broadcasted_iota(jnp.int32, (n, n), 0)
    cols = lax.broadcasted_iota(jnp.int32, (n, n), 1)
    eye = rows == cols
    pt = p.T
    re = jnp.where(rows <= cols, p, pt)
    im = jnp.where(rows > cols, p, jnp.where(rows < cols, -pt, 0.0))
    squares = 2.0 * p * p - jnp.where(eye, p * p, 0.0)
    low = load_ratio * power_ref[0:1, 0:1]
    high = jnp.sqrt(jnp.sum(squares, keepdims=True)) + low
    alpha = 2.0 / (low + high)
    rho = ((high - low) / (high + low))[0, 0]
    full = jnp.where(eye, re + low, re)
    ar[...] = full
    ai[...] = im
    e_r = jnp.where(eye, 1.0, 0.0) - alpha * full
    e_i = -alpha * im
    (rh, rl), (ih, il) = halves(e_r), halves(e_i)
    top = jnp.concatenate([rh, ih], 1)
    rest = jnp.concatenate([rl, il], 1)
    by_real = three(rh, rl, top, rest)
    by_imag = three(ih, il, top, rest)
    mu = 2.0 / (2.0 - rho * rho)
    er[...] = mu * (by_real[:, :n] - by_imag[:, n:]) + jnp.where(eye, 1.0 - mu, 0.0)
    ei[...] = mu * (by_real[:, n:] + by_imag[:, :n])
    xr[...] = (mu * alpha) * (jnp.where(eye, 1.0, 0.0) + e_r)
    xi[...] = (mu * alpha) * e_i
    rho = rho * rho * mu * 0.5

    for arrival in arrivals:
        arrival.start()

    def step(exact, rho):
        e_r, e_i, x_r, x_i = er[...], ei[...], xr[...], xi[...]
        if exact:
            (rh, rl), (ih, il) = halves(e_r), halves(e_i)
            (xh, xl), (yh, yl) = halves(x_r), halves(x_i)
            top = jnp.concatenate([rh, ih, xh, yh], 1)
            rest = jnp.concatenate([rl, il, xl, yl], 1)
            by_real = three(rh, rl, top, rest)
            by_imag = three(ih, il, top, rest)
        else:
            both = jnp.concatenate([v.astype(bf16) for v in (e_r, e_i, x_r, x_i)], 1)
            by_real = dot(both[:, :n], both)
            by_imag = dot(both[:, n : 2 * n], both)
        mu = 2.0 / (2.0 - rho * rho)
        er[...] = mu * (by_real[:, :n] - by_imag[:, n : 2 * n]) + jnp.where(eye, 1.0 - mu, 0.0)
        ei[...] = mu * (by_real[:, n : 2 * n] + by_imag[:, :n])
        xr[...] = mu * (x_r + by_real[:, 2 * n : 3 * n] - by_imag[:, 3 * n :])
        xi[...] = mu * (x_i + by_real[:, 3 * n :] + by_imag[:, 2 * n : 3 * n])
        return rho * rho * mu * 0.5

    rho = lax.while_loop(lambda r: r > 0.5, functools.partial(step, True), rho)
    rho = lax.while_loop(lambda r: r > 0.05, functools.partial(step, False), rho)

    @pl.when(rho > 1e-3)
    def _():
        e_r, e_i, x_r, x_i = er[...], ei[...], xr[...], xi[...]
        both = jnp.concatenate([x_r.astype(bf16), x_i.astype(bf16)], 1)
        by_real = dot(e_r.astype(bf16), both)
        by_imag = dot(e_i.astype(bf16), both)
        xr[...] = x_r + by_real[:, :n] - by_imag[:, n:]
        xi[...] = x_i + by_real[:, n:] + by_imag[:, :n]

    s_r, s_i = sr_ref[...], si_ref[...]
    (xh, xl), (yh, yl) = halves(xr[...]), halves(xi[...])
    top = jnp.concatenate([jnp.concatenate([xh, -yh], 1), jnp.concatenate([yh, xh], 1)], 0)
    rest = jnp.concatenate([jnp.concatenate([xl, -yl], 1), jnp.concatenate([yl, xl], 1)], 0)

    def applied(v_r, v_i):
        (rh, rl), (ih, il) = halves(v_r), halves(v_i)
        return three(jnp.concatenate([rh, ih], 1), jnp.concatenate([rl, il], 1), top, rest)

    w = applied(s_r, s_i)
    a = jnp.concatenate(
        [jnp.concatenate([ar[...], -ai[...]], 1), jnp.concatenate([ai[...], ar[...]], 1)], 0
    )
    back = jnp.dot(w, a, precision=lax.Precision.HIGHEST, preferred_element_type=f32)
    w = w + applied(s_r - back[:, :n], s_i - back[:, n:])
    w_r, w_i = w[:, :n], w[:, n:]
    gain = jnp.sum(s_r * w_r + s_i * w_i, axis=1, keepdims=True)
    t_r = (w_r / gain).astype(bf16)
    t_i = (w_i / gain).astype(bf16)
    taps = jnp.concatenate([jnp.concatenate([t_r, t_i], 1), jnp.concatenate([-t_i, t_r], 1)], 0)
    leaving = []
    for i, span in enumerate(spans):
        arrivals[i].wait()
        out_ref[:, span] = lax.dot_general(
            taps, x_ref[span], (((1,), (1,)), ((), ())), preferred_element_type=f32
        ).astype(bf16)
        leaving.append(pltpu.make_async_copy(out_ref.at[:, span], out_hbm.at[:, span], sems.at[1, i]))
        leaving[i].start()
    for copy in leaving:
        copy.wait()


def solve_and_filter(gathered, noise, steer_real, steer_imag, snaps):
    m, n = steer_real.shape
    cells, width = snaps.shape
    return pl.pallas_call(
        solve_body,
        in_specs=[pl.BlockSpec(memory_space=pltpu.VMEM)] * 4 + [pl.BlockSpec(memory_space=pl.ANY)],
        out_specs=pl.BlockSpec(memory_space=pl.ANY),
        out_shape=jax.ShapeDtypeStruct((2 * m, cells), bf16),
        scratch_shapes=[pltpu.VMEM((cells, width), bf16), pltpu.VMEM((2 * m, cells), bf16)]
        + [pltpu.VMEM((n, n), f32)] * 6
        + [pltpu.SemaphoreType.DMA((2, cells // FILTER_CELLS))],
        name="solve",
    )(gathered, noise, steer_real, steer_imag, snaps)


def steering(doppler, chans, pulses):
    index = jnp.arange(chans * pulses)
    chan = (index // pulses).astype(f32)
    pulse = (index % pulses).astype(f32)
    freq = doppler.astype(f32) / NDOPP - 0.5
    phase = 2.0 * jnp.pi * (look_freq * chan[None, :] + pulse[None, :] * freq[:, None])
    scale = jnp.sqrt(f32(chans * pulses))
    return jnp.cos(phase) / scale, jnp.sin(phase) / scale


def exchange(x, axis):
    return lax.all_to_all(x, axis, split_axis=0, concat_axis=0, tiled=True)


def sum_of_few(x, axis):
    size = lax.axis_size(axis)
    stride = 1
    while stride < size:
        x = x + lax.ppermute(x, axis, [(i, i ^ stride) for i in range(size)])
        stride *= 2
    return x


def per_device(snapshots, training, doppler):
    snaps = snapshots[0]
    cells, width = snaps.shape
    half = width // 2
    parts = lax.axis_size("cells")
    sums = local_gram(snaps, training.reshape(1, cells))
    own = exchange(sums.reshape(parts, 1, -1), "cells").sum(axis=0)
    count = 8 * half
    lines = own[0, :count].reshape(-1, LANES)
    trace = own[:, count:]
    gathered = exchange(jnp.broadcast_to(lines, (parts, *lines.shape)), "cells")
    power = sum_of_few(trace, "bins")
    noise = power / (lax.axis_size("bins") * half)
    steer_real, steer_imag = steering(doppler[0], CHANNELS, PULSES)
    inputs = (gathered.reshape(-1, LANES), noise, steer_real, steer_imag)
    inputs = [pltpu.with_memory_space_constraint(v, pltpu.VMEM) for v in inputs]
    return solve_and_filter(*inputs, snaps)[None]


def solution(mesh):
    in_specs = (P("bins", "cells", None), P("cells"), P("bins", None))
    out_specs = P("bins", None, "cells")
    return jax.shard_map(
        per_device, mesh=mesh, in_specs=in_specs, out_specs=out_specs, check_vma=False
    )
```

```python
import functools

import jax
import jax.numpy as jnp
from jax import lax
from jax.experimental import pallas as pl
from jax.experimental.pallas import tpu as pltpu
from jax.sharding import PartitionSpec as P

CHANNELS = 16
PULSES = 16
NDOPP = 1024
LANES = 128
GRAM_CELLS = 2048
GRAM_AHEAD = 4
FILTER_CELLS = 1024

load_ratio = 0.5
look_freq = 0.125

bf16 = jnp.bfloat16
f32 = jnp.float32


def dot(a, b):
    return jnp.dot(a, b, preferred_element_type=f32)


def gram_body(x_hbm, keep_hbm, out_ref, x_ref, keep_ref, acc_ref, sems):
    cells, width = x_ref.shape
    half = width // 2
    steps = cells // GRAM_CELLS

    def copy(step):
        rows = pl.ds(pl.multiple_of(step * GRAM_CELLS, GRAM_CELLS), GRAM_CELLS)
        return pltpu.make_async_copy(x_hbm.at[rows], x_ref.at[rows], sems.at[step])

    copy(0).start()
    keeps = pltpu.make_async_copy(keep_hbm, keep_ref, sems.at[steps])
    keeps.start()
    for step in range(1, GRAM_AHEAD):
        copy(step).start()
    acc_ref[...] = jnp.zeros_like(acc_ref)

    def add(step, _):
        @pl.when(step + GRAM_AHEAD < steps)
        def _():
            copy(step + GRAM_AHEAD).start()

        copy(step).wait()
        start = pl.multiple_of(step * GRAM_CELLS, GRAM_CELLS)
        x = x_ref[pl.ds(start, GRAM_CELLS)]
        keep = keep_ref[:, pl.ds(start, GRAM_CELLS)]
        kept = x.T * keep.astype(f32).astype(bf16)
        by_real = dot(kept, x[:, :half])
        by_imag = dot(kept[half:], x[:, half:])
        acc_ref[:half] += by_real[:half] + by_imag
        acc_ref[half:] += by_real[half:]
        return 0

    keeps.wait()
    lax.fori_loop(0, steps, add, 0)
    real = acc_ref[:half]
    cross = acc_ref[half:]
    imag = cross - cross.T
    rows = lax.broadcasted_iota(jnp.int32, (half, half), 0)
    cols = lax.broadcasted_iota(jnp.int32, (half, half), 1)
    packed = jnp.where(rows <= cols, real, imag)
    trace = jnp.sum(jnp.where(rows == cols, real, 0.0), keepdims=True)
    parts = half // 8
    span = out_ref.shape[0] // parts
    for part in range(parts):
        lines = packed[8 * part : 8 * part + 8]
        for block in range(half // LANES):
            out_ref[span * part + 8 * block : span * part + 8 * block + 8] = lines[
                :, LANES * block : LANES * block + LANES
            ]
        out_ref[span * part + span - 1 : span * part + span] = jnp.broadcast_to(trace, (1, LANES))


def local_gram(snaps, keep):
    cells, width = snaps.shape
    half = width // 2
    span = 8 * half // LANES + 1
    return pl.pallas_call(
        gram_body,
        in_specs=[pl.BlockSpec(memory_space=pl.ANY)] * 2,
        out_specs=pl.BlockSpec(memory_space=pltpu.VMEM),
        out_shape=jax.ShapeDtypeStruct((half // 8 * span, LANES), f32),
        scratch_shapes=[
            pltpu.VMEM((cells, width), bf16),
            pltpu.VMEM((1, cells), jnp.int32),
            pltpu.VMEM((width, half), f32),
            pltpu.SemaphoreType.DMA((cells // GRAM_CELLS + 1,)),
        ],
        name="gram",
    )(snaps, keep)


def halves(x):
    top = x.astype(bf16)
    return top, (x - top.astype(f32)).astype(bf16)


def three(ah, al, bh, bl):
    return dot(jnp.concatenate([ah, ah, al], 1), jnp.concatenate([bh, bl, bh], 0))


def solve_body(
    gathered_ref, power_ref, sr_ref, si_ref, x_hbm, out_hbm, x_ref, out_ref, ar, ai, er, ei, xr, xi, sems
):
    n = ar.shape[0]
    cells = x_ref.shape[0]
    chunks = cells // FILTER_CELLS
    spans = [pl.ds(FILTER_CELLS * i, FILTER_CELLS) for i in range(chunks)]
    arrival = pltpu.make_async_copy(x_hbm, x_ref, sems.at[0])
    lines = gathered_ref[...].reshape(n // 8, n // LANES, 8, LANES)
    p = jnp.concatenate([lines[:, b].reshape(n, LANES) for b in range(n // LANES)], 1)
    rows = lax.broadcasted_iota(jnp.int32, (n, n), 0)
    cols = lax.broadcasted_iota(jnp.int32, (n, n), 1)
    eye = rows == cols
    pt = p.T
    re = jnp.where(rows <= cols, p, pt)
    im = jnp.where(rows > cols, p, jnp.where(rows < cols, -pt, 0.0))
    squares = 2.0 * p * p - jnp.where(eye, p * p, 0.0)
    low = load_ratio * power_ref[0:1, 0:1]
    high = jnp.sqrt(jnp.sum(squares, keepdims=True)) + low
    alpha = 2.0 / (low + high)
    rho = ((high - low) / (high + low))[0, 0]
    full = jnp.where(eye, re + low, re)
    ar[...] = full
    ai[...] = im
    e_r = jnp.where(eye, 1.0, 0.0) - alpha * full
    e_i = -alpha * im
    reals, imags, sums = [three(a, b, a, b) for a, b in map(halves, (e_r, e_i, e_r + e_i))]
    mu = 2.0 / (2.0 - rho * rho)
    er[...] = mu * (reals - imags) + jnp.where(eye, 1.0 - mu, 0.0)
    ei[...] = mu * (sums - (reals + imags))
    xr[...] = (mu * alpha) * (jnp.where(eye, 1.0, 0.0) + e_r)
    xi[...] = (mu * alpha) * e_i
    rho = rho * rho * mu * 0.5

    arrival.start()

    def step(exact, rho):
        e_r, e_i, x_r, x_i = er[...], ei[...], xr[...], xi[...]
        if exact:
            (rh, rl), (ih, il), (gh, gl) = halves(e_r), halves(e_i), halves(e_r + e_i)
            (xh, xl), (yh, yl), (zh, zl) = halves(x_r), halves(x_i), halves(x_r + x_i)
            operands = [(rh, rl, xh, xl), (ih, il, yh, yl), (gh, gl, zh, zl)]
            reals, imags, sums = [
                three(a, b, jnp.concatenate([a, c], 1), jnp.concatenate([b, d], 1))
                for a, b, c, d in operands
            ]
            real_part = reals - imags
            imag_part = sums - (reals + imags)
        else:
            both = jnp.concatenate([v.astype(bf16) for v in (e_r, e_i, x_r, x_i)], 1)
            by_real = dot(both[:, :n], both)
            by_imag = dot(both[:, n : 2 * n], both)
            real_part = jnp.concatenate(
                [by_real[:, :n] - by_imag[:, n : 2 * n], by_real[:, 2 * n : 3 * n] - by_imag[:, 3 * n :]], 1
            )
            imag_part = jnp.concatenate(
                [by_real[:, n : 2 * n] + by_imag[:, :n], by_real[:, 3 * n :] + by_imag[:, 2 * n : 3 * n]], 1
            )
        mu = 2.0 / (2.0 - rho * rho)
        er[...] = mu * real_part[:, :n] + jnp.where(eye, 1.0 - mu, 0.0)
        ei[...] = mu * imag_part[:, :n]
        xr[...] = mu * (x_r + real_part[:, n:])
        xi[...] = mu * (x_i + imag_part[:, n:])
        return rho * rho * mu * 0.5

    rho = lax.while_loop(lambda r: r > 0.5, functools.partial(step, True), rho)
    rho = lax.while_loop(lambda r: r > 0.05, functools.partial(step, False), rho)

    @pl.when(rho > 1e-3)
    def _():
        e_r, e_i, x_r, x_i = er[...], ei[...], xr[...], xi[...]
        both = jnp.concatenate([x_r.astype(bf16), x_i.astype(bf16)], 1)
        by_real = dot(e_r.astype(bf16), both)
        by_imag = dot(e_i.astype(bf16), both)
        xr[...] = x_r + by_real[:, :n] - by_imag[:, n:]
        xi[...] = x_i + by_real[:, n:] + by_imag[:, :n]

    s_r, s_i = sr_ref[...], si_ref[...]
    (xh, xl), (yh, yl) = halves(xr[...]), halves(xi[...])
    top = jnp.concatenate([jnp.concatenate([xh, -yh], 1), jnp.concatenate([yh, xh], 1)], 0)
    rest = jnp.concatenate([jnp.concatenate([xl, -yl], 1), jnp.concatenate([yl, xl], 1)], 0)

    def applied(v_r, v_i):
        (rh, rl), (ih, il) = halves(v_r), halves(v_i)
        return three(jnp.concatenate([rh, ih], 1), jnp.concatenate([rl, il], 1), top, rest)

    w = applied(s_r, s_i)
    a = jnp.concatenate(
        [jnp.concatenate([ar[...], -ai[...]], 1), jnp.concatenate([ai[...], ar[...]], 1)], 0
    )
    back = jnp.dot(w, a, precision=lax.Precision.HIGHEST, preferred_element_type=f32)
    w = w + applied(s_r - back[:, :n], s_i - back[:, n:])
    w_r, w_i = w[:, :n], w[:, n:]
    gain = jnp.sum(s_r * w_r + s_i * w_i, axis=1, keepdims=True)
    t_r = (w_r / gain).astype(bf16)
    t_i = (w_i / gain).astype(bf16)
    taps = jnp.concatenate([jnp.concatenate([t_r, t_i], 1), jnp.concatenate([-t_i, t_r], 1)], 0)
    arrival.wait()
    leaving = []
    for i, span in enumerate(spans):
        out_ref[:, span] = lax.dot_general(
            taps, x_ref[span], (((1,), (1,)), ((), ())), preferred_element_type=f32
        ).astype(bf16)
        leaving.append(pltpu.make_async_copy(out_ref.at[:, span], out_hbm.at[:, span], sems.at[1 + i]))
        leaving[i].start()
    for copy in leaving:
        copy.wait()


def solve_and_filter(gathered, noise, steer_real, steer_imag, snaps):
    m, n = steer_real.shape
    cells, width = snaps.shape
    return pl.pallas_call(
        solve_body,
        in_specs=[pl.BlockSpec(memory_space=pltpu.VMEM)] * 4 + [pl.BlockSpec(memory_space=pl.ANY)],
        out_specs=pl.BlockSpec(memory_space=pl.ANY),
        out_shape=jax.ShapeDtypeStruct((2 * m, cells), bf16),
        scratch_shapes=[pltpu.VMEM((cells, width), bf16), pltpu.VMEM((2 * m, cells), bf16)]
        + [pltpu.VMEM((n, n), f32)] * 6
        + [pltpu.SemaphoreType.DMA((1 + cells // FILTER_CELLS,))],
        name="solve",
    )(gathered, noise, steer_real, steer_imag, snaps)


def steering(doppler, chans, pulses):
    index = jnp.arange(chans * pulses)
    chan = (index // pulses).astype(f32)
    pulse = (index % pulses).astype(f32)
    freq = doppler.astype(f32) / NDOPP - 0.5
    phase = 2.0 * jnp.pi * (look_freq * chan[None, :] + pulse[None, :] * freq[:, None])
    scale = jnp.sqrt(f32(chans * pulses))
    return jnp.cos(phase) / scale, jnp.sin(phase) / scale


def exchange(x, axis):
    return lax.all_to_all(x, axis, split_axis=0, concat_axis=0, tiled=True)


def sum_of_few(x, axis):
    size = lax.axis_size(axis)
    stride = 1
    while stride < size:
        x = x + lax.ppermute(x, axis, [(i, i ^ stride) for i in range(size)])
        stride *= 2
    return x


def per_device(snapshots, training, doppler):
    snaps = snapshots[0]
    cells, width = snaps.shape
    half = width // 2
    parts = lax.axis_size("cells")
    sums = local_gram(snaps, training.reshape(1, cells))
    own = exchange(sums.reshape(parts, 1, -1), "cells").sum(axis=0)
    count = 8 * half
    lines = own[0, :count].reshape(-1, LANES)
    trace = own[:, count:]
    gathered = exchange(jnp.broadcast_to(lines, (parts, *lines.shape)), "cells")
    power = sum_of_few(trace, "bins")
    noise = power / (lax.axis_size("bins") * half)
    steer_real, steer_imag = steering(doppler[0], CHANNELS, PULSES)
    inputs = (gathered.reshape(-1, LANES), noise, steer_real, steer_imag)
    inputs = [pltpu.with_memory_space_constraint(v, pltpu.VMEM) for v in inputs]
    return solve_and_filter(*inputs, snaps)[None]


def solution(mesh):
    in_specs = (P("bins", "cells", None), P("cells"), P("bins", None))
    out_specs = P("bins", None, "cells")
    return jax.shard_map(
        per_device, mesh=mesh, in_specs=in_specs, out_specs=out_specs, check_vma=False
    )
```

```python
import functools

import jax
import jax.numpy as jnp
from jax import lax
from jax.experimental import pallas as pl
from jax.experimental.pallas import tpu as pltpu
from jax.sharding import PartitionSpec as P


CHANNELS = 16
PULSES = 16
NDOPP = 1024
LANES = 128
GRAM_CELLS = 2048
GRAM_AHEAD = 4
FILTER_CELLS = 1024

load_ratio = 0.5
look_freq = 0.125

bf16 = jnp.bfloat16
f32 = jnp.float32


def dot(a, b):
    return jnp.dot(a, b, preferred_element_type=f32)


def gram_body(x_hbm, keep_hbm, out_ref, x_ref, keep_ref, acc_ref, sems):
    cells, width = x_ref.shape
    half = width // 2
    steps = cells // GRAM_CELLS

    def copy(step):
        rows = pl.ds(pl.multiple_of(step * GRAM_CELLS, GRAM_CELLS), GRAM_CELLS)
        return pltpu.make_async_copy(x_hbm.at[rows], x_ref.at[rows], sems.at[step])

    copy(0).start()
    keeps = pltpu.make_async_copy(keep_hbm, keep_ref, sems.at[steps])
    keeps.start()
    for step in range(1, GRAM_AHEAD):
        copy(step).start()
    acc_ref[...] = jnp.zeros_like(acc_ref)

    def add(step, _):
        @pl.when(step + GRAM_AHEAD < steps)
        def _():
            copy(step + GRAM_AHEAD).start()

        copy(step).wait()
        start = pl.multiple_of(step * GRAM_CELLS, GRAM_CELLS)
        x = x_ref[pl.ds(start, GRAM_CELLS)]
        keep = keep_ref[:, pl.ds(start, GRAM_CELLS)]
        kept = x.T * keep.astype(f32).astype(bf16)
        by_real = dot(kept, x[:, :half])
        by_imag = dot(kept[half:], x[:, half:])
        acc_ref[:half] += by_real[:half] + by_imag
        acc_ref[half:] += by_real[half:]
        return 0

    keeps.wait()
    lax.fori_loop(0, steps, add, 0)
    real = acc_ref[:half]
    cross = acc_ref[half:]
    imag = cross - cross.T
    rows = lax.broadcasted_iota(jnp.int32, (half, half), 0)
    cols = lax.broadcasted_iota(jnp.int32, (half, half), 1)
    packed = jnp.where(rows <= cols, real, imag)
    trace = jnp.sum(jnp.where(rows == cols, real, 0.0), keepdims=True)
    parts = half // 8
    span = out_ref.shape[0] // parts
    for part in range(parts):
        lines = packed[8 * part : 8 * part + 8]
        for block in range(half // LANES):
            out_ref[span * part + 8 * block : span * part + 8 * block + 8] = lines[
                :, LANES * block : LANES * block + LANES
            ]
        out_ref[span * part + span - 1 : span * part + span] = jnp.broadcast_to(trace, (1, LANES))


def local_gram(snaps, keep):
    cells, width = snaps.shape
    half = width // 2
    span = 8 * half // LANES + 1
    return pl.pallas_call(
        gram_body,
        in_specs=[pl.BlockSpec(memory_space=pl.ANY)] * 2,
        out_specs=pl.BlockSpec(memory_space=pltpu.VMEM),
        out_shape=jax.ShapeDtypeStruct((half // 8 * span, LANES), f32),
        scratch_shapes=[
            pltpu.VMEM((cells, width), bf16),
            pltpu.VMEM((1, cells), jnp.int32),
            pltpu.VMEM((width, half), f32),
            pltpu.SemaphoreType.DMA((cells // GRAM_CELLS + 1,)),
        ],
        name="gram",
    )(snaps, keep)


def halves(x):
    top = x.astype(bf16)
    return top, (x - top.astype(f32)).astype(bf16)


def three(ah, al, bh, bl):
    return dot(jnp.concatenate([ah, ah, al], 1), jnp.concatenate([bh, bl, bh], 0))


def solve_body(
    gathered_ref, power_ref, sr_ref, si_ref, x_hbm, out_hbm, x_ref, out_ref, ar, ai, er, ei, xr, xi, sems
):
    n = ar.shape[0]
    cells = x_ref.shape[0]
    chunks = cells // FILTER_CELLS
    spans = [pl.ds(FILTER_CELLS * i, FILTER_CELLS) for i in range(chunks)]
    arrival = pltpu.make_async_copy(x_hbm, x_ref, sems.at[0])
    lines = gathered_ref[...].reshape(n // 8, n // LANES, 8, LANES)
    p = jnp.concatenate([lines[:, b].reshape(n, LANES) for b in range(n // LANES)], 1)
    rows = lax.broadcasted_iota(jnp.int32, (n, n), 0)
    cols = lax.broadcasted_iota(jnp.int32, (n, n), 1)
    eye = rows == cols
    pt = p.T
    re = jnp.where(rows <= cols, p, pt)
    im = jnp.where(rows > cols, p, jnp.where(rows < cols, -pt, 0.0))
    squares = 2.0 * p * p - jnp.where(eye, p * p, 0.0)
    low = load_ratio * power_ref[0:1, 0:1]
    high = jnp.sqrt(jnp.sum(squares, keepdims=True)) + low
    alpha = 2.0 / (low + high)
    rho = spread = ((high - low) / (high + low))[0, 0]
    full = jnp.where(eye, re + low, re)
    ar[...] = full
    ai[...] = im
    e_r = jnp.where(eye, 1.0, 0.0) - alpha * full
    e_i = -alpha * im
    reals, imags, sums = [three(a, b, a, b) for a, b in map(halves, (e_r, e_i, e_r + e_i))]
    mu = 2.0 / (2.0 - rho * rho)
    er[...] = mu * (reals - imags) + jnp.where(eye, 1.0 - mu, 0.0)
    ei[...] = mu * (sums - (reals + imags))
    xr[...] = (mu * alpha) * (jnp.where(eye, 1.0, 0.0) + e_r)
    xi[...] = (mu * alpha) * e_i
    rho = rho * rho * mu * 0.5

    arrival.start()

    def step(exact, rho):
        e_r, e_i, x_r, x_i = er[...], ei[...], xr[...], xi[...]
        if exact:
            (rh, rl), (ih, il), (gh, gl) = halves(e_r), halves(e_i), halves(e_r + e_i)
            (xh, xl), (yh, yl), (zh, zl) = halves(x_r), halves(x_i), halves(x_r + x_i)
            operands = [(rh, rl, xh, xl), (ih, il, yh, yl), (gh, gl, zh, zl)]
            reals, imags, sums = [
                three(a, b, jnp.concatenate([a, c], 1), jnp.concatenate([b, d], 1))
                for a, b, c, d in operands
            ]
            real_part = reals - imags
            imag_part = sums - (reals + imags)
        else:
            both = jnp.concatenate([v.astype(bf16) for v in (e_r, e_i, x_r, x_i)], 1)
            by_real = dot(both[:, :n], both)
            by_imag = dot(both[:, n : 2 * n], both)
            real_part = jnp.concatenate(
                [by_real[:, :n] - by_imag[:, n : 2 * n], by_real[:, 2 * n : 3 * n] - by_imag[:, 3 * n :]], 1
            )
            imag_part = jnp.concatenate(
                [by_real[:, n : 2 * n] + by_imag[:, :n], by_real[:, 3 * n :] + by_imag[:, 2 * n : 3 * n]], 1
            )
        mu = 2.0 / (2.0 - rho * rho)
        er[...] = mu * real_part[:, :n] + jnp.where(eye, 1.0 - mu, 0.0)
        ei[...] = mu * imag_part[:, :n]
        xr[...] = mu * (x_r + real_part[:, n:])
        xi[...] = mu * (x_i + imag_part[:, n:])
        return rho * rho * mu * 0.5

    rho = lax.while_loop(lambda r: r > 0.5, functools.partial(step, True), rho)
    rho = lax.while_loop(lambda r: r > 0.05, functools.partial(step, False), rho)

    @pl.when(rho > 1e-3)
    def _():
        e_r, e_i, x_r, x_i = er[...], ei[...], xr[...], xi[...]
        both = jnp.concatenate([x_r.astype(bf16), x_i.astype(bf16)], 1)
        by_real = dot(e_r.astype(bf16), both)
        by_imag = dot(e_i.astype(bf16), both)
        xr[...] = x_r + by_real[:, :n] - by_imag[:, n:]
        xi[...] = x_i + by_real[:, n:] + by_imag[:, :n]

    s_r, s_i = sr_ref[...], si_ref[...]
    (xh, xl), (yh, yl) = halves(xr[...]), halves(xi[...])
    top = jnp.concatenate([jnp.concatenate([xh, -yh], 1), jnp.concatenate([yh, xh], 1)], 0)
    rest = jnp.concatenate([jnp.concatenate([xl, -yl], 1), jnp.concatenate([yl, xl], 1)], 0)

    def applied(v_r, v_i):
        (rh, rl), (ih, il) = halves(v_r), halves(v_i)
        return three(jnp.concatenate([rh, ih], 1), jnp.concatenate([rl, il], 1), top, rest)

    def corrected(w):
        a = jnp.concatenate(
            [jnp.concatenate([ar[...], -ai[...]], 1), jnp.concatenate([ai[...], ar[...]], 1)], 0
        )
        back = jnp.dot(w, a, precision=lax.Precision.HIGHEST, preferred_element_type=f32)
        return w + applied(s_r - back[:, :n], s_i - back[:, n:])

    m = s_r.shape[0]
    w = corrected(applied(s_r, s_i))
    er[:m] = w[:, :n]
    er[m:] = w[:, n:]

    @pl.when(spread > 0.995)
    def _():
        w = corrected(jnp.concatenate([er[:m], er[m:]], 1))
        er[:m] = w[:, :n]
        er[m:] = w[:, n:]

    w_r, w_i = er[:m], er[m:]
    gain = jnp.sum(s_r * w_r + s_i * w_i, axis=1, keepdims=True)
    t_r = (w_r / gain).astype(bf16)
    t_i = (w_i / gain).astype(bf16)
    taps = jnp.concatenate([jnp.concatenate([t_r, t_i], 1), jnp.concatenate([-t_i, t_r], 1)], 0)
    arrival.wait()
    leaving = []
    for i, span in enumerate(spans):
        out_ref[:, span] = lax.dot_general(
            taps, x_ref[span], (((1,), (1,)), ((), ())), preferred_element_type=f32
        ).astype(bf16)
        leaving.append(pltpu.make_async_copy(out_ref.at[:, span], out_hbm.at[:, span], sems.at[1 + i]))
        leaving[i].start()
    for copy in leaving:
        copy.wait()


def solve_and_filter(gathered, noise, steer_real, steer_imag, snaps):
    m, n = steer_real.shape
    cells, width = snaps.shape
    return pl.pallas_call(
        solve_body,
        in_specs=[pl.BlockSpec(memory_space=pltpu.VMEM)] * 4 + [pl.BlockSpec(memory_space=pl.ANY)],
        out_specs=pl.BlockSpec(memory_space=pl.ANY),
        out_shape=jax.ShapeDtypeStruct((2 * m, cells), bf16),
        scratch_shapes=[pltpu.VMEM((cells, width), bf16), pltpu.VMEM((2 * m, cells), bf16)]
        + [pltpu.VMEM((n, n), f32)] * 6
        + [pltpu.SemaphoreType.DMA((1 + cells // FILTER_CELLS,))],
        name="solve",
    )(gathered, noise, steer_real, steer_imag, snaps)


def steering(doppler, chans, pulses):
    index = jnp.arange(chans * pulses)
    chan = (index // pulses).astype(f32)
    pulse = (index % pulses).astype(f32)
    freq = doppler.astype(f32) / NDOPP - 0.5
    phase = 2.0 * jnp.pi * (look_freq * chan[None, :] + pulse[None, :] * freq[:, None])
    scale = jnp.sqrt(f32(chans * pulses))
    return jnp.cos(phase) / scale, jnp.sin(phase) / scale


def exchange(x, axis):
    return lax.all_to_all(x, axis, split_axis=0, concat_axis=0, tiled=True)


def sum_of_few(x, axis):
    size = lax.axis_size(axis)
    stride = 1
    while stride < size:
        x = x + lax.ppermute(x, axis, [(i, i ^ stride) for i in range(size)])
        stride *= 2
    return x


def per_device(snapshots, training, doppler):
    snaps = snapshots[0]
    cells, width = snaps.shape
    half = width // 2
    parts = lax.axis_size("cells")
    sums = local_gram(snaps, training.reshape(1, cells))
    own = exchange(sums.reshape(parts, 1, -1), "cells").sum(axis=0)
    count = 8 * half
    lines = own[0, :count].reshape(-1, LANES)
    trace = own[:, count:]
    gathered = exchange(jnp.broadcast_to(lines, (parts, *lines.shape)), "cells")
    power = sum_of_few(trace, "bins")
    noise = power / (lax.axis_size("bins") * half)
    steer_real, steer_imag = steering(doppler[0], CHANNELS, PULSES)
    inputs = (gathered.reshape(-1, LANES), noise, steer_real, steer_imag)
    inputs = [pltpu.with_memory_space_constraint(v, pltpu.VMEM) for v in inputs]
    return solve_and_filter(*inputs, snaps)[None]


def solution(mesh):
    in_specs = (P("bins", "cells", None), P("cells"), P("bins", None))
    out_specs = P("bins", None, "cells")
    return jax.shard_map(
        per_device, mesh=mesh, in_specs=in_specs, out_specs=out_specs, check_vma=False
    )
```
